32 devices in a mesh: dp: 4 (over y, core), seq: 8 (over z, x).
Axes of the slice: x: 2, y: 2, z: 4, core: 2. Of those that a mesh axis runs over, the one named last changes fastest.
Arguments:
- tokens: bfloat16 [32768, 2048], P(('dp', 'seq')), parts along dimension 0, may hold values from -6 to 6
- chosen: int32 [4096], P('dp'), parts along dimension 0, may hold values from 0 to 8191, as said below
- gates: float32 [4096], P('dp'), parts along dimension 0, may hold values from 0.5 to 2
- w_query: bfloat16 [2048, 1024], P('seq'), may hold values from -1.8561553 to 1.8561553
- w_key: bfloat16 [2048, 256], P('seq'), may hold values from -0.088388348 to 0.088388348
- w_value: bfloat16 [2048, 256], P('seq'), may hold values from -0.125 to 0.125
- w_out: bfloat16 [1024, 2048], P(None, 'seq'), may hold values from -0.5 to 0.5
Outputs:
- mixed: bfloat16 [32768, 2048], P(('dp', 'seq')), parts along dimension 0
The draws below stay inside these ranges and needn't reach their ends.
There are 4 independent parts, one for each index of `dp`. The reference program is written for one: setup_inputs(seed, part) draws one part's arguments, and reference() takes and returns one part's arrays. A program takes and returns all parts, laid end to end along the dimension named above; an argument that names none is the same for every part. Nothing has to cross between parts.
Inputs may be any that keep to these rules, and one draw needn't show every extreme that they name: `chosen`: distinct positions in increasing order; at most 256 of them lie in one device's 1024 consecutive positions, and exactly 256 lie in some device's positions.
All inputs are finite; a program needn't handle non-finite values.
Results may differ from the reference program's by a relative error of at most 0.006.
Values may be sent and summed in bfloat16 or wider, within the bound.
No kernel may reach another device: no remote copies, remote signals or barrier semaphores. Data moves between devices by JAX's collectives and lax.ppermute only.
A program may use at most 128 MiB of HBM per device.

```python
import math
import jax
import jax.numpy as jnp
from jax import lax

D = 2048
HEADS = 8
KV_HEADS = 2
HEAD_DIM = 128
TOK_DEV = 1024
ROWS_DEV = 128
TOKENS = 8192
CHOSEN = 1024
N_SEQ = 8


def draw_chosen(key, part):
    lifts = jax.random.randint(jax.random.fold_in(key, 1), (N_SEQ,), 0, ROWS_DEV + 1)
    heavy = jax.random.randint(jax.random.fold_in(key, 2), (), 0, N_SEQ)
    order = jnp.arange(N_SEQ, dtype=jnp.int32)
    lifts = jnp.where(order == heavy, ROWS_DEV, lifts)
    lifts = jnp.where(order == (heavy + N_SEQ - 1) % N_SEQ, 0, lifts)
    counts = ROWS_DEV + lifts - jnp.roll(lifts, 1)
    subkeys = jax.random.split(jax.random.fold_in(key, 3), N_SEQ)
    ranks = jax.vmap(lambda single: jax.random.permutation(single, TOK_DEV))(subkeys)
    flags = (ranks < counts[:, None]).reshape(-1)
    return jnp.nonzero(flags, size=CHOSEN)[0].astype(jnp.int32)


def shared_base(key):
    raw = jax.random.normal(jax.random.fold_in(key, 11), (D, KV_HEADS * HEAD_DIM), jnp.float32)
    return jnp.clip(raw, -4.0, 4.0) * D ** (-0.5)


def draw_w_key(key, part):
    return shared_base(key).astype(jnp.bfloat16)


def draw_w_query(key, part):
    raw = jax.random.normal(jax.random.fold_in(key, 12), (D, HEADS * HEAD_DIM), jnp.float32)
    noise = jnp.clip(raw, -4.0, 4.0) * 2.0 * D ** (-0.5)
    return noise.astype(jnp.bfloat16)


def steps_of(rng, dims, cuts, least, top_value):
    gain = 1.0
    for position, shards_of in cuts:
        steps = jax.random.uniform(jax.random.fold_in(jax.random.fold_in(rng, 6), position), (shards_of,), jnp.float32, least / len(cuts), top_value / len(cuts))
        gain = gain * jnp.repeat(jnp.exp(steps), dims[position] // shards_of).reshape((-1,) + (1,) * (len(dims) - 1 - position))
    return gain


def bell_draw(rng, dims, spread, limit, cuts=(), kind=jnp.bfloat16):
    drawn = spread * jax.random.normal(rng, dims, jnp.float32)
    if cuts:
        drawn = drawn * steps_of(rng, dims, cuts, -0.22, 0.18)
    return jnp.clip(drawn, -limit, limit).astype(kind)


def setup_inputs(seed: int = 0, part: int = 0) -> dict:
    splits = jax.random.split(jax.random.key(seed), 8)
    part_splits = jax.random.split(jax.random.fold_in(splits[7], part), 8)
    return {
        "tokens": bell_draw(part_splits[0], (TOKENS, D), 1.0, 6.0, ((0, 8),)),
        "chosen": draw_chosen(jax.random.fold_in(jax.random.fold_in(splits[7], part), 71), part),
        "gates": jnp.clip(jax.random.uniform(part_splits[2], (CHOSEN,), jnp.float32, 0.5, 2.0), 0.5, 2.0),
        "w_query": draw_w_query(jax.random.fold_in(splits[7], 71), part),
        "w_key": draw_w_key(jax.random.fold_in(splits[7], 71), part),
        "w_value": bell_draw(splits[5], (D, KV_HEADS * HEAD_DIM), D ** -0.5, 0.125, ((0, 8),)),
        "w_out": bell_draw(splits[6], (HEADS * HEAD_DIM, D), (HEADS * HEAD_DIM // 9) ** -0.5, 0.5, ((1, 8),)),
    }


neg_fill = -1e+30

def reference(tokens, chosen, gates, w_query, w_key, w_value, w_out):
    picked_total = chosen.shape[0]
    group_size = HEADS // KV_HEADS
    block_rows = math.gcd(picked_total, 512)
    picked = tokens[chosen].astype(jnp.float32)
    normed = (picked * lax.rsqrt(lax.optimization_barrier(jnp.mean(picked * picked, axis=1, keepdims=True)) + 1e-06)).astype(jnp.bfloat16)
    query_matrix = (jnp.dot(normed, w_query, preferred_element_type=jnp.float32) * HEAD_DIM ** (-0.5)).astype(jnp.bfloat16)
    keys_all = jnp.dot(normed, w_key, preferred_element_type=jnp.float32).astype(jnp.bfloat16)
    values = jnp.dot(normed, w_value, preferred_element_type=jnp.float32).astype(jnp.bfloat16)
    query_matrix = lax.optimization_barrier(query_matrix).astype(jnp.float32)
    keys_expanded = lax.optimization_barrier(keys_all).astype(jnp.float32).reshape(picked_total, KV_HEADS, HEAD_DIM)
    values_expanded = lax.optimization_barrier(values).astype(jnp.float32).reshape(picked_total, KV_HEADS, HEAD_DIM)
    blocks = query_matrix.reshape(picked_total // block_rows, block_rows, KV_HEADS, group_size, HEAD_DIM)
    firsts = (jnp.arange(picked_total // block_rows, dtype=jnp.int32) * block_rows).astype(jnp.int32)
    key_order = jnp.arange(picked_total, dtype=jnp.int32)

    def one_block(inputs):
        query_tile, first_row = inputs
        logit_scores = jnp.einsum('qjfh,ujh->jfqu', query_tile, keys_expanded)
        query_order = first_row + jnp.arange(block_rows, dtype=jnp.int32)
        allowed = key_order[None, :] <= query_order[:, None]
        logit_scores = jnp.where(allowed, logit_scores, neg_fill)
        top_score = lax.optimization_barrier(jnp.max(logit_scores, axis=-1, keepdims=True))
        probs = jnp.where(allowed, jnp.exp(logit_scores - top_score), 0.0)
        totals = lax.optimization_barrier(jnp.sum(probs, axis=-1))
        softmax_weights = lax.optimization_barrier(probs.astype(jnp.bfloat16)).astype(jnp.float32)
        summed_total = jnp.einsum('yoih,hyf->yoif', softmax_weights, values_expanded)
        attended = summed_total / totals[..., None]
        return jnp.transpose(attended, (2, 0, 1, 3)).reshape(block_rows, HEADS * HEAD_DIM)
    attended = lax.map(one_block, (blocks, firsts)).reshape(picked_total, HEADS * HEAD_DIM).astype(jnp.bfloat16)
    block_out = jnp.dot(attended, w_out, preferred_element_type=jnp.float32).astype(jnp.bfloat16)
    block_wide = lax.optimization_barrier(block_out).astype(jnp.float32)
    mixed = tokens.astype(jnp.float32).at[chosen].add(gates[:, None] * block_wide)
    return mixed.astype(jnp.bfloat16)
```

```python
import functools

import jax
import jax.numpy as jnp
from jax import lax
from jax.experimental import pallas as pl
from jax.experimental.pallas import tpu as pltpu
from jax.sharding import PartitionSpec as P

HEADS = 8
KV_HEADS = 2
HEAD_DIM = 128
MOST_OWN = 256
CORES = 2
INNER = 2
ALIGN = 16
KEY_BLOCK = 256

neg_fill = -1e30
never = 1 << 30


VMEM = pl.BlockSpec(memory_space=pltpu.VMEM)
SMEM = pl.BlockSpec(memory_space=pltpu.SMEM)


def cost(flops, moved):
    return pl.CostEstimate(flops=flops, bytes_accessed=moved, transcendentals=0)


def pick_kernel(shards, order_ref, spot_ref, tokens_ref, out_ref, wide_ref):
    rows, tok_rows = spot_ref.shape[0], tokens_ref.shape[0]
    width = tokens_ref.shape[1] // shards
    steps = lax.broadcasted_iota(jnp.int32, (rows, tok_rows), 1)
    select = jnp.where(spot_ref[...] == steps, 1.0, 0.0).astype(jnp.bfloat16)
    total = jnp.zeros((rows, 1), jnp.float32)
    for j in range(shards):
        part = jnp.dot(
            select, tokens_ref[:, j * width : (j + 1) * width], preferred_element_type=jnp.float32
        )
        wide_ref[j] = part
        total = total + jnp.sum(part * part, axis=1, keepdims=True)
    scale = lax.rsqrt(total / tokens_ref.shape[1] + 1e-06)
    for j in range(shards):
        out_ref[:, j * width : (j + 1) * width] = (wide_ref[order_ref[j]] * scale).astype(
            jnp.bfloat16
        )


def pick_rows(tokens, spot, order):
    shards = order.shape[0]
    tok_rows, model_width = tokens.shape
    width = model_width // shards
    rows = spot.shape[0]
    if width % 128:
        steps = jnp.arange(tok_rows, dtype=jnp.int32)
        select = (spot[:, None] == steps[None, :]).astype(jnp.bfloat16)
        wide = jnp.dot(select, tokens, preferred_element_type=jnp.float32)
        scale = lax.rsqrt(jnp.mean(wide * wide, axis=1, keepdims=True) + 1e-06)
        normed = (wide * scale).astype(jnp.bfloat16).reshape(rows, shards, width)
        return normed[:, order].reshape(rows, model_width)
    return pl.pallas_call(
        functools.partial(pick_kernel, shards),
        out_shape=jax.ShapeDtypeStruct((rows, model_width), jnp.bfloat16),
        in_specs=[SMEM, VMEM, VMEM],
        out_specs=VMEM,
        scratch_shapes=[pltpu.VMEM((shards, rows, width), jnp.float32)],
        cost_estimate=cost(2 * rows * tok_rows * model_width, 2 * tok_rows * model_width),
        name="pick_rows",
    )(order, spot[:, None], tokens)


def attend_kernel(sources, pieces, heads_here, table_ref, query_ref, *refs):
    kv_refs, (out_ref, keys_ref, values_ref) = refs[:sources], refs[sources:]
    rows = query_ref.shape[1]
    wide = KV_HEADS * HEAD_DIM
    room = keys_ref.shape[0]
    key_at = pl.multiple_of(table_ref[3, 0] * wide, wide)
    value_at = pl.multiple_of(wide - table_ref[3, 0] * wide, wide)
    first_query = table_ref[3, 1]
    keys_ref[...] = jnp.zeros_like(keys_ref)
    values_ref[...] = jnp.zeros_like(values_ref)
    spots = lax.broadcasted_iota(jnp.int32, (1, room), 1)
    key_ids = jnp.full((1, room), never, jnp.int32)
    offset = jnp.int32(0)
    for j in range(sources):
        count, start = table_ref[0, j], table_ref[1, j]

        @pl.when(count > 0)
        def _(j=j, offset=offset):
            at = pl.multiple_of(offset, ALIGN)
            keys_ref[pl.ds(at, rows), :] = kv_refs[j][:, pl.ds(key_at, wide)]
            values_ref[pl.ds(at, rows), :] = kv_refs[j][:, pl.ds(value_at, wide)]

        local = spots - offset
        key_ids = jnp.where((local >= 0) & (local < count), start + local, key_ids)
        offset = offset + (count + ALIGN - 1) // ALIGN * ALIGN
    blocks = (offset + KEY_BLOCK - 1) // KEY_BLOCK
    ids = [key_ids[:, b * KEY_BLOCK : (b + 1) * KEY_BLOCK] for b in range(room // KEY_BLOCK)]
    tall = heads_here * rows
    query_ids = first_query + lax.broadcasted_iota(jnp.int32, (tall, 1), 0) % rows

    def one_piece(t, carry):
        head = table_ref[2, t]
        lanes = pl.ds(pl.multiple_of(head * HEAD_DIM, HEAD_DIM), HEAD_DIM)
        query = jnp.concatenate(
            [query_ref[t, :, h * HEAD_DIM : (h + 1) * HEAD_DIM] for h in range(heads_here)], axis=0
        )

        def one_block(b, state):
            top, total, mixed = state
            at = pl.ds(pl.multiple_of(b * KEY_BLOCK, KEY_BLOCK), KEY_BLOCK)
            scores = lax.dot_general(
                query, keys_ref[at, lanes], (((1,), (1,)), ((), ())), preferred_element_type=jnp.float32
            )
            here = ids[0]
            for k in range(1, len(ids)):
                here = jnp.where(b == k, ids[k], here)
            allowed = here <= query_ids
            scores = jnp.where(allowed, scores, neg_fill)
            fresh = jnp.maximum(top, jnp.max(scores, axis=1, keepdims=True))
            probs = jnp.where(allowed, jnp.exp(scores - fresh), 0.0)
            shrink = jnp.exp(top - fresh)
            total = total * shrink + jnp.sum(probs, axis=1, keepdims=True)
            mixed = mixed * shrink + jnp.dot(
                probs.astype(jnp.bfloat16), values_ref[at, lanes], preferred_element_type=jnp.float32
            )
            return fresh, total, mixed

        start = (
            jnp.full((tall, 1), neg_fill, jnp.float32),
            jnp.zeros((tall, 1), jnp.float32),
            jnp.zeros((tall, HEAD_DIM), jnp.float32),
        )
        _, total, mixed = lax.fori_loop(0, blocks, one_block, start)
        attended = (mixed / jnp.maximum(total, 1e-30)).astype(jnp.bfloat16)
        for h in range(heads_here):
            out_ref[t, :, h * HEAD_DIM : (h + 1) * HEAD_DIM] = attended[h * rows : (h + 1) * rows]
        return carry

    lax.fori_loop(0, pieces, one_piece, 0)


def attend(table, queries, blocks, most_keys):
    pieces, rows, wide = queries.shape
    sources = len(blocks)
    room = -(-(most_keys + sources * (ALIGN - 1)) // KEY_BLOCK) * KEY_BLOCK + MOST_OWN
    return pl.pallas_call(
        functools.partial(attend_kernel, sources, pieces, wide // HEAD_DIM),
        out_shape=jax.ShapeDtypeStruct(queries.shape, jnp.bfloat16),
        in_specs=[SMEM] + [VMEM] * (1 + sources),
        out_specs=VMEM,
        scratch_shapes=[pltpu.VMEM((room, KV_HEADS * HEAD_DIM), jnp.bfloat16)] * 2,
        cost_estimate=cost(4 * rows * pieces * wide * room, 4 * rows * wide * sources),
        name="attend",
    )(table, queries, *blocks)


def query_kernel(width, normed_ref, *refs):
    weight_refs, out_ref = refs[:-1], refs[-1]
    for t, weight_ref in enumerate(weight_refs):
        wide = jnp.dot(
            normed_ref[...], weight_ref[:, :width], preferred_element_type=jnp.float32
        )
        out_ref[t] = (wide * HEAD_DIM ** (-0.5)).astype(jnp.bfloat16)


def project_queries(normed, weights, width):
    rows = normed.shape[0]
    return pl.pallas_call(
        functools.partial(query_kernel, width),
        out_shape=jax.ShapeDtypeStruct((len(weights), rows, width), jnp.bfloat16),
        in_specs=[VMEM] * (1 + len(weights)),
        out_specs=VMEM,
        cost_estimate=cost(2 * rows * normed.shape[1] * width * len(weights), normed.size * 2),
        name="project_queries",
    )(normed, *weights)


def output_kernel(order_ref, attended_ref, select_ref, gates_ref, tokens_ref, *refs):
    weight_refs, out_ref = refs[:-1], refs[-1]
    total = None
    for t, weight_ref in enumerate(weight_refs):
        part = jnp.dot(attended_ref[t], weight_ref[...], preferred_element_type=jnp.float32)
        total = part if total is None else total + part
    spread = jnp.dot(
        select_ref[...], total.astype(jnp.bfloat16), preferred_element_type=jnp.float32
    )
    out_ref[...] = (tokens_ref[...].astype(jnp.float32) + gates_ref[...] * spread).astype(
        jnp.bfloat16
    )


def add_output(order, attended, select, lift, tokens, weights, lane):
    shards = order.shape[0]
    pieces, rows, wide = attended.shape
    tok_rows, model_width = tokens.shape
    width = model_width // shards
    if width % 128:
        total = sum(
            jnp.einsum(
                "ak,jkn->ajn",
                attended[t],
                w.reshape(shards, wide, width),
                preferred_element_type=jnp.float32,
            )
            for t, w in enumerate(weights)
        )
        back = jnp.zeros((shards,), jnp.int32).at[order].set(jnp.arange(shards, dtype=jnp.int32))
        block_out = total.astype(jnp.bfloat16)[:, back].reshape(rows, model_width)
        spread = jnp.dot(select, block_out, preferred_element_type=jnp.float32)
        return (tokens.astype(jnp.float32) + lift * spread).astype(jnp.bfloat16)
    grid_spec = pltpu.PrefetchScalarGridSpec(
        num_scalar_prefetch=1,
        grid=(shards,),
        in_specs=[
            pl.BlockSpec((pieces, rows, wide), lambda j, order: (0, 0, 0)),
            pl.BlockSpec((tok_rows, rows), lambda j, order: (0, 0)),
            pl.BlockSpec((tok_rows, 1), lambda j, order: (0, 0)),
            pl.BlockSpec((tok_rows, width), lambda j, order: (0, order[j])),
        ]
        + [pl.BlockSpec((wide, width), lambda j, order: (j, lane))] * pieces,
        out_specs=pl.BlockSpec((tok_rows, width), lambda j, order: (0, order[j])),
    )
    return pl.pallas_call(
        output_kernel,
        out_shape=jax.ShapeDtypeStruct(tokens.shape, jnp.bfloat16),
        grid_spec=grid_spec,
        cost_estimate=cost(2 * rows * model_width * (tok_rows + wide * pieces), 4 * tokens.size),
        name="add_output",
    )(order, attended, select, lift, tokens, *weights)


def per_device(tokens, chosen, gates, w_query, w_key, w_value, w_out):
    shards, copies = lax.axis_size("seq"), lax.axis_size("dp")
    me, copy_of = lax.axis_index("seq"), lax.axis_index("dp")
    outer, planes = shards // INNER, copies // CORES
    my_outer, my_inner = me // INNER, me % INNER
    my_plane, my_core = copy_of // CORES, copy_of % CORES
    tok_rows = tokens.shape[0]
    picked_total = chosen.shape[0]

    def along_outer(x, step):
        pairs = [(s, (s + step * INNER) % shards) for s in range(shards)]
        return lax.ppermute(x, "seq", pairs)

    def toward_later(x, step):
        return lax.ppermute(x, "seq", [(s, s + step * INNER) for s in range(shards - step * INNER)])

    def along_inner(x, step):
        pairs = [(s, s - s % INNER + (s + step) % INNER) for s in range(shards)]
        return lax.ppermute(x, "seq", pairs)

    def along_planes(x, step):
        return lax.ppermute(x, "dp", [(q, (q + step * CORES) % copies) for q in range(copies)])

    def other_core(x):
        return lax.ppermute(x, "dp", [(q, q ^ 1) for q in range(copies)])

    rel_inner, rel_outer = jnp.divmod(jnp.arange(shards, dtype=jnp.int32), outer)
    order = (my_outer - rel_outer) % outer * INNER + (my_inner - rel_inner) % INNER

    near = [jnp.where(my_core == 0, w_key, w_value)]
    near += [along_outer(near[0], k) for k in range(1, outer)]
    kv_weights = near + [along_inner(x, f) for f in range(1, INNER) for x in near]

    part = HEADS * HEAD_DIM // copies
    query_part = lax.dynamic_slice_in_dim(w_query, copy_of * part, part, 1)
    out_part = lax.dynamic_slice_in_dim(w_out, copy_of * part, part, 0)
    packed = query_part.shape == out_part.shape
    chains = [jnp.concatenate([query_part, out_part], 1)] if packed else [query_part, out_part]

    def gather_pieces(own):
        column = jnp.concatenate([own] + [along_outer(own, k) for k in range(1, outer)], 0)
        whole = jnp.concatenate([column] + [along_inner(column, f) for f in range(1, INNER)], 0)
        mine = [whole] + [along_planes(whole, g) for g in range(1, planes)]
        return mine + [other_core(x) for x in mine]

    base = me * tok_rows
    starts = jnp.sum((chosen[None, :] < (jnp.arange(shards + 1) * tok_rows)[:, None]), axis=1, dtype=jnp.int32)
    counts = starts[1:] - starts[:-1]
    padded = jnp.concatenate([chosen, jnp.full((MOST_OWN,), never, jnp.int32)])
    padded_gates = jnp.concatenate([gates, jnp.zeros((MOST_OWN,), jnp.float32)])
    my_start = starts[me]
    spot = lax.dynamic_slice_in_dim(padded, my_start, MOST_OWN, 0) - base
    spot = jnp.where(spot < tok_rows, spot, -1)
    own_gates = lax.dynamic_slice_in_dim(padded_gates, my_start, MOST_OWN, 0)
    taken = spot[None, :] == jnp.arange(tok_rows, dtype=jnp.int32)[:, None]
    select = taken.astype(jnp.bfloat16)
    lift = jnp.sum(jnp.where(taken, own_gates[None, :], 0.0), axis=1, keepdims=True)

    normed = pick_rows(tokens, spot, order)
    partner = other_core(normed)
    both = jnp.concatenate([normed, partner], 0)
    kv_whole = jnp.concatenate(kv_weights, 0)
    projected = jnp.dot(both, kv_whole, preferred_element_type=jnp.float32).astype(jnp.bfloat16)
    from_core = other_core(projected[MOST_OWN:])
    own_kv = jnp.concatenate([projected[:MOST_OWN], from_core], 1)
    column = [own_kv] + [toward_later(own_kv, k) for k in range(1, outer)]
    kv_blocks = column + [along_inner(x, f) for f in range(1, INNER) for x in column]

    gathered = [gather_pieces(own) for own in chains]
    query_weights, out_weights = gathered[0], gathered[-1]
    queries = project_queries(normed, query_weights, part)

    core_step, plane_step = jnp.divmod(jnp.arange(copies, dtype=jnp.int32), planes)
    piece = (my_plane - plane_step) % planes * CORES + (my_core + core_step) % CORES
    kv_head = piece * part // (HEADS // KV_HEADS * HEAD_DIM)
    source = order
    seen = jnp.where(source <= me, counts[source], 0)
    wide = max(shards, copies)
    table = jnp.stack(
        [
            jnp.pad(seen, (0, wide - shards)),
            jnp.pad(starts[source], (0, wide - shards)),
            jnp.pad(kv_head, (0, wide - copies)),
            jnp.pad(jnp.stack([my_core, my_start]), (0, wide - 2)),
        ]
    )
    attended = attend(table, queries, kv_blocks, picked_total)
    return add_output(order, attended, select, lift, tokens, out_weights, 1 if packed else 0)


def solution(mesh):
    return jax.shard_map(
        per_device,
        mesh=mesh,
        in_specs=(
            P(("dp", "seq"), None),
            P("dp"),
            P("dp"),
            P("seq", None),
            P("seq", None),
            P("seq", None),
            P(None, "seq"),
        ),
        out_specs=P(("dp", "seq"), None),
        check_vma=False,
    )
```
